32 devices in a mesh: row: 4 (over y, x), col: 4 (over z), depth: 2 (over core).
Axes of the slice: x: 2, y: 2, z: 4, core: 2. Of those that a mesh axis runs over, the one named last changes fastest.
Arguments:
- orbitals: bfloat16 [2, 1024, 2, 4096], P(None, ('row', 'col'), 'depth'), may hold values from -20 to 20
- potential: float32 [2, 4096], P('depth'), may hold values from -6 to 6
Outputs:
- intersection: float32 [1024, 2, 1024], P(('row', 'depth'), None, 'col')
- applied: bfloat16 [2, 1024, 2, 4096], P(None, ('row', 'col'), 'depth')
The draws below stay inside these ranges and needn't reach their ends.
All inputs are finite; a program needn't handle non-finite values.
Results may differ from the reference program's by a relative error of at most 0.001.
Values may be sent and summed in bfloat16 or wider, within the bound.
A program may use at most 128 MiB of HBM per device.

```python
import jax
import jax.numpy as jnp
from jax import lax

NORB = 1024
NX = 64
NZ = 2
NYX = 4096


def draw_orbitals(key, part):
    base_key = jax.random.fold_in(key, 11)
    first, second = jax.random.split(base_key, 2)
    shape = (2, NORB, NZ, NYX)
    noise = jnp.clip(jax.random.normal(first, shape, jnp.float32), -4.0, 4.0)
    scales = jnp.exp(jax.random.uniform(second, (1, NORB, 1, 1), jnp.float32, -0.69, 0.69))
    mixed = noise + 0.6 * jnp.roll(noise, 1, axis=1) + 0.4 * jnp.roll(noise, 37, axis=1)
    total = mixed * scales
    return jnp.clip(total, -20.0, 20.0).astype(jnp.bfloat16)


def block_levels(own_key, dims, shards, low, largest):
    def one(axis_at, shards_of):
        draws = jax.random.uniform(jax.random.fold_in(jax.random.fold_in(own_key, 6), axis_at), (shards_of,), jnp.float32, low / len(shards), largest / len(shards))
        return jnp.repeat(jnp.exp(draws), dims[axis_at] // shards_of).reshape((-1,) + (1,) * (len(dims) - axis_at - 1))

    gain = one(*shards[0])
    for cut in shards[1:]:
        gain = gain * one(*cut)
    return gain


def gaussian(own_key, dims, deviation, bound, cuts=(), dtype=jnp.bfloat16):
    level = block_levels(own_key, dims, cuts, -0.22, 0.18) if cuts else 1.0
    array = jax.random.normal(own_key, dims, jnp.float32) * deviation * level
    return jnp.minimum(jnp.maximum(array, -bound), bound).astype(dtype)


def setup_inputs(seed: int = 0) -> dict:
    arg_keys = jax.random.split(jax.random.key(seed), 3)
    return {
        "orbitals": draw_orbitals(jax.random.fold_in(arg_keys[2], 71), 0),
        "potential": gaussian(arg_keys[1], (NZ, NYX), 1.0, 6.0, ((0, 2),), jnp.float32),
    }


def apply_operator(field, potential):
    flat_cells = field.shape[-1]
    xpos = jnp.arange(flat_cells) % NX
    below = jnp.roll(field, 1, axis=2)
    above = jnp.roll(field, -1, axis=2)
    yminus = jnp.roll(field, NX, axis=3)
    yplus = jnp.roll(field, -NX, axis=3)
    xminus = jnp.where(xpos == 0, jnp.roll(field, 1 - NX, axis=3), jnp.roll(field, 1, axis=3))
    xplus = jnp.where(xpos == NX - 1, jnp.roll(field, NX - 1, axis=3), jnp.roll(field, -1, axis=3))
    lap = below + above + yminus + yplus + xminus + xplus - 6.0 * field
    return -0.5 * lap + potential[None, None] * field


def reference(orbitals, potential):
    wide = orbitals.astype(jnp.float32)
    cells = NZ * NYX
    real_part = wide[0].reshape(NORB, cells)
    imag_part = wide[1].reshape(NORB, cells)
    dvol = 1.0 / cells
    high = lax.Precision.HIGHEST
    sreal = jnp.dot(real_part, real_part.T, precision=high) + jnp.dot(imag_part, imag_part.T, precision=high)
    simag = jnp.dot(real_part, imag_part.T, precision=high) - jnp.dot(imag_part, real_part.T, precision=high)
    intersection = jnp.stack([sreal * dvol, simag * dvol], axis=1)
    applied = apply_operator(wide, potential).astype(jnp.bfloat16)
    return intersection, applied
```

```python
import functools

import jax
import jax.numpy as jnp
from jax import lax
from jax.experimental import pallas as pl
from jax.experimental.pallas import tpu as pltpu
from jax.sharding import PartitionSpec as P

NX = 64
MESH = pl.DeviceIdType.MESH


def with_halo(block, sides, width):
    for axis, dim in sides:
        count = lax.axis_size(axis)
        forward = [(i, i + 1) for i in range(count - 1)]
        forward.append((count - 1, 0))
        backward = [(target, source) for source, target in forward]
        low = lax.ppermute(
            lax.slice_in_dim(block, block.shape[dim] - width, None, axis=dim), axis, forward
        )
        high = lax.ppermute(lax.slice_in_dim(block, 0, width, axis=dim), axis, backward)
        block = jnp.concatenate([low, block, high], axis=dim)
    return block


def apply_operator(padded, potential):
    center = padded[:, :, 1:-1].astype(jnp.float32)
    below = padded[:, :, :-2].astype(jnp.float32)
    above = padded[:, :, 2:].astype(jnp.float32)
    flat_cells = center.shape[-1]
    xpos = jnp.arange(flat_cells) % NX
    yminus = jnp.roll(center, NX, axis=3)
    yplus = jnp.roll(center, -NX, axis=3)
    xminus = jnp.where(xpos == 0, jnp.roll(center, 1 - NX, axis=3), jnp.roll(center, 1, axis=3))
    xplus = jnp.where(
        xpos == NX - 1, jnp.roll(center, NX - 1, axis=3), jnp.roll(center, -1, axis=3)
    )
    lap = below + above + yminus + yplus + xminus + xplus - 6.0 * center
    return (-0.5 * lap + potential[None, None] * center).astype(jnp.bfloat16)


def contract(left, right):
    return lax.dot_general(
        left, right, (((1,), (1,)), ((), ())), preferred_element_type=jnp.float32
    )


def shards(orbitals, potential):
    parts, orbs, planes, cells = orbitals.shape
    flat = orbitals.reshape(parts, orbs, planes * cells)
    panel = lax.all_gather(flat, "col", axis=1, tiled=True)
    other = lax.all_gather(flat, "row", axis=1, tiled=True)
    padded = with_halo(orbitals, (("depth", 2),), 1)
    applied = apply_operator(padded, potential)
    dvol = 1.0 / (planes * lax.axis_size("depth") * cells)
    tile_cols = other.shape[1]
    real_rows = panel[0]
    imag_rows = panel[1]
    sreal = contract(real_rows, other[0]) + contract(imag_rows, other[1])
    simag = contract(real_rows, other[1]) - contract(imag_rows, other[0])
    summed = lax.psum_scatter(
        dvol * jnp.concatenate([sreal, simag], axis=1), "depth", scatter_dimension=0, tiled=True
    )
    intersection = summed.reshape(summed.shape[0], 2, tile_cols)
    intersection = lax.all_to_all(intersection, "col", split_axis=2, concat_axis=2, tiled=True)
    return (intersection, applied)


def flip(a, b):
    low = lax.rem(lax.rem(a, 2) + lax.rem(b, 2), 2)
    high = lax.rem(lax.div(a, 2) + lax.div(b, 2), 2)
    return 2 * high + low


def stencil(orb, halo, pot, out):
    parts, orbs, cells = orb.shape
    step = 16
    xpos = lax.broadcasted_iota(jnp.int32, (step, cells), 1) % NX
    first, last = xpos == 0, xpos == NX - 1

    def body(i, carry):
        part = lax.div(i, orbs // step)
        rows = pl.ds(pl.multiple_of(lax.rem(i, orbs // step) * step, step), step)
        center = orb[part, rows, :].astype(jnp.float32)
        side = halo[part, rows, :].astype(jnp.float32)
        right = pltpu.roll(center, 1, 1)
        left = pltpu.roll(center, cells - 1, 1)
        yminus = pltpu.roll(center, NX, 1)
        yplus = pltpu.roll(center, cells - NX, 1)
        xminus = jnp.where(first, pltpu.roll(right, cells - NX, 1), right)
        xplus = jnp.where(last, pltpu.roll(left, NX, 1), left)
        lap = side + side + yminus + yplus + xminus + xplus - 6.0 * center
        out[part, rows, :] = (-0.5 * lap + pot[0:1, :] * center).astype(out.dtype)
        return carry

    lax.fori_loop(0, parts * (orbs // step), body, 0)


def kernel(dvol, orb, pot, inter, applied, halo, panel, acc, give, take, land,
           hs, hr, ls, zs, zr, xs, xr, ds, dr, gs, gr, rs, rr):
    r, c, d = lax.axis_index("row"), lax.axis_index("col"), lax.axis_index("depth")
    parts, orbs, cells = orb.shape
    quarter = cells // 4
    half = acc.shape[2]
    peer = (r, c, 1 - d)
    zdev = [None] + [(r, flip(c, k), d) for k in (1, 2, 3)]
    xdev = [None] + [(flip(r, k), c, d) for k in (1, 2)]

    barrier = pltpu.get_barrier_semaphore()
    friends = [peer] + zdev[1:] + xdev[1:]
    for dev in friends:
        pl.semaphore_signal(barrier, inc=1, device_id=dev, device_id_type=MESH)
    pl.semaphore_wait(barrier, len(friends))

    def send(src, dst, ssem, rsem, dev):
        return pltpu.make_async_remote_copy(
            src_ref=src, dst_ref=dst, send_sem=ssem, recv_sem=rsem,
            device_id=dev, device_id_type=MESH,
        )

    def lanes(k):
        return pl.ds(pl.multiple_of(k * quarter, quarter), quarter)

    def block(j, k):
        return panel.at[j, :, pl.ds(pl.multiple_of(k * orbs, orbs), orbs), :]

    zsend = {}
    for k in (3, 2, 1):
        zsend[k] = send(orb.at[:, :, lanes(flip(c, k))], block(0, c), zs.at[k], zr.at[k], zdev[k])
        zsend[k].start()
    xsend = {}
    for j in (1, 2):
        xsend[0, j] = send(orb.at[:, :, lanes(c)], block(j, c), xs.at[0, j], xr.at[0, j], xdev[j])
        xsend[0, j].start()
    edge = send(orb, halo, hs, hr, peer)
    edge.start()
    local = pltpu.make_async_copy(orb.at[:, :, lanes(c)], block(0, c), ls)
    local.start()

    edge.wait()
    stencil(orb, halo, pot, applied)
    local.wait()

    for k in (1, 2, 3):
        zsend[k].wait_recv()
        for j in (1, 2):
            xsend[k, j] = send(block(0, flip(c, k)), block(j, flip(c, k)),
                               xs.at[k, j], xr.at[k, j], xdev[j])
            xsend[k, j].start()

    def tile(slot, jl, jr):
        for part in (0, 1):
            for mine in (0, 1):
                at = d if mine else 1 - d
                rows = pl.ds(pl.multiple_of(at * half, half), half)
                a, b = panel[jl, 0, rows, :], panel[jl, 1, rows, :]
                if part == 0:
                    s = contract(a, panel[jr, 0]) + contract(b, panel[jr, 1])
                else:
                    s = contract(a, panel[jr, 1]) - contract(b, panel[jr, 0])
                if mine:
                    acc[slot, part] = s
                else:
                    give[slot, part] = s
        cp = send(give.at[slot], take.at[slot], ds.at[slot], dr.at[slot], peer)
        cp.start()
        return cp

    def ship(t):
        to = flip(r, jnp.int32(t))
        gap = flip(c, to)
        return to, gap, send(acc.at[t], land.at[gap], gs.at[t], gr.at[gap], (r, to, d))

    def start_ship(t):
        to, gap, cp = ship(t)

        @pl.when(to != c)
        def _():
            cp.start()

    pair = {0: tile(0, 0, 0)}
    for k in (0, 1, 2, 3):
        xsend[k, 1].wait_recv()
        xsend[k, 2].wait_recv()
    pair[4] = tile(4, 1, 2)
    pair[1] = tile(1, 0, 1)
    pair[2] = tile(2, 0, 2)
    pair[4].wait_recv()
    acc[4] += take[4]
    cross = send(acc.at[4], acc.at[3], rs, rr, xdev[1])
    cross.start()
    for t in (0, 1, 2):
        pair[t].wait_recv()
        acc[t] += take[t]
        start_ship(t)
    cross.wait_recv()
    start_ship(3)

    total = acc[flip(r, c)]
    for k in (1, 2, 3):
        send(acc.at[0], land.at[k], gs.at[0], gr.at[k], zdev[k]).wait_recv()
        total = total + land[k]
    inter[...] = total * dvol

    for cp in [edge, cross] + list(pair.values()) + list(zsend.values()) + list(xsend.values()):
        if cp is not edge:
            cp.wait_send()
    for t in (0, 1, 2, 3):
        to, gap, cp = ship(t)

        @pl.when(to != c)
        def _():
            cp.wait_send()


def exchange(orbitals, potential):
    parts, orbs, planes, cells = orbitals.shape
    rows = orbs * lax.axis_size("col")
    half = rows // 2
    dvol = 1.0 / (planes * lax.axis_size("depth") * cells)
    vmem = pl.BlockSpec(memory_space=pltpu.VMEM)
    dma = pltpu.SemaphoreType.DMA
    inter, applied = pl.pallas_call(
        functools.partial(kernel, dvol),
        out_shape=(
            jax.ShapeDtypeStruct((2, half, rows), jnp.float32),
            jax.ShapeDtypeStruct((parts, orbs, cells), jnp.bfloat16),
        ),
        in_specs=[vmem, vmem],
        out_specs=(vmem, vmem),
        scratch_shapes=[
            pltpu.VMEM((parts, orbs, cells), jnp.bfloat16),
            pltpu.VMEM((3, parts, rows, cells // 4), jnp.bfloat16),
            pltpu.VMEM((5, 2, half, rows), jnp.float32),
            pltpu.VMEM((5, 2, half, rows), jnp.float32),
            pltpu.VMEM((5, 2, half, rows), jnp.float32),
            pltpu.VMEM((4, 2, half, rows), jnp.float32),
            dma, dma, dma, dma((4,)), dma((4,)), dma((4, 3)), dma((4, 3)),
            dma((5,)), dma((5,)), dma((4,)), dma((4,)), dma, dma,
        ],
        compiler_params=pltpu.CompilerParams(
            collective_id=0, has_side_effects=True, vmem_limit_bytes=60000000
        ),
        name="overlap",
    )(orbitals.reshape(parts, orbs, cells), potential)
    return jnp.transpose(inter, (1, 0, 2)), applied.reshape(orbitals.shape)


def solution(mesh):
    in_specs = (P(None, ("row", "col"), "depth", None), P("depth", None))
    out_specs = (P(("row", "depth"), None, "col"), P(None, ("row", "col"), "depth", None))
    sizes = tuple(mesh.shape[axis] for axis in ("row", "col", "depth"))
    body = exchange if sizes == (4, 4, 2) else shards
    return jax.shard_map(body, mesh=mesh, in_specs=in_specs, out_specs=out_specs, check_vma=False)
```

```python
import functools

import jax
import jax.numpy as jnp
from jax import lax
from jax.experimental import pallas as pl
from jax.experimental.pallas import tpu as pltpu
from jax.sharding import PartitionSpec as P

NX = 64
MESH = pl.DeviceIdType.MESH


def with_halo(block, sides, width):
    for axis, dim in sides:
        count = lax.axis_size(axis)
        forward = [(i, i + 1) for i in range(count - 1)]
        forward.append((count - 1, 0))
        backward = [(target, source) for source, target in forward]
        low = lax.ppermute(
            lax.slice_in_dim(block, block.shape[dim] - width, None, axis=dim), axis, forward
        )
        high = lax.ppermute(lax.slice_in_dim(block, 0, width, axis=dim), axis, backward)
        block = jnp.concatenate([low, block, high], axis=dim)
    return block


def apply_operator(padded, potential):
    center = padded[:, :, 1:-1].astype(jnp.float32)
    below = padded[:, :, :-2].astype(jnp.float32)
    above = padded[:, :, 2:].astype(jnp.float32)
    flat_cells = center.shape[-1]
    xpos = jnp.arange(flat_cells) % NX
    yminus = jnp.roll(center, NX, axis=3)
    yplus = jnp.roll(center, -NX, axis=3)
    xminus = jnp.where(xpos == 0, jnp.roll(center, 1 - NX, axis=3), jnp.roll(center, 1, axis=3))
    xplus = jnp.where(
        xpos == NX - 1, jnp.roll(center, NX - 1, axis=3), jnp.roll(center, -1, axis=3)
    )
    lap = below + above + yminus + yplus + xminus + xplus - 6.0 * center
    return (-0.5 * lap + potential[None, None] * center).astype(jnp.bfloat16)


def contract(left, right):
    return lax.dot_general(
        left, right, (((1,), (1,)), ((), ())), preferred_element_type=jnp.float32
    )


def shards(orbitals, potential):
    parts, orbs, planes, cells = orbitals.shape
    flat = orbitals.reshape(parts, orbs, planes * cells)
    panel = lax.all_gather(flat, "col", axis=1, tiled=True)
    other = lax.all_gather(flat, "row", axis=1, tiled=True)
    padded = with_halo(orbitals, (("depth", 2),), 1)
    applied = apply_operator(padded, potential)
    dvol = 1.0 / (planes * lax.axis_size("depth") * cells)
    tile_cols = other.shape[1]
    real_rows = panel[0]
    imag_rows = panel[1]
    sreal = contract(real_rows, other[0]) + contract(imag_rows, other[1])
    simag = contract(real_rows, other[1]) - contract(imag_rows, other[0])
    summed = lax.psum_scatter(
        dvol * jnp.concatenate([sreal, simag], axis=1), "depth", scatter_dimension=0, tiled=True
    )
    intersection = summed.reshape(summed.shape[0], 2, tile_cols)
    intersection = lax.all_to_all(intersection, "col", split_axis=2, concat_axis=2, tiled=True)
    return (intersection, applied)


def flip(a, b):
    low = lax.rem(lax.rem(a, 2) + lax.rem(b, 2), 2)
    high = lax.rem(lax.div(a, 2) + lax.div(b, 2), 2)
    return 2 * high + low


def stencil(orb, halo, pot, out):
    parts, orbs, cells = orb.shape
    step = 16
    xpos = lax.broadcasted_iota(jnp.int32, (step, cells), 1) % NX
    first, last = xpos == 0, xpos == NX - 1

    def body(i, carry):
        part = lax.div(i, orbs // step)
        rows = pl.ds(pl.multiple_of(lax.rem(i, orbs // step) * step, step), step)
        center = orb[part, rows, :].astype(jnp.float32)
        side = halo[part, rows, :].astype(jnp.float32)
        right = pltpu.roll(center, 1, 1)
        left = pltpu.roll(center, cells - 1, 1)
        yminus = pltpu.roll(center, NX, 1)
        yplus = pltpu.roll(center, cells - NX, 1)
        xminus = jnp.where(first, pltpu.roll(right, cells - NX, 1), right)
        xplus = jnp.where(last, pltpu.roll(left, NX, 1), left)
        lap = side + side + yminus + yplus + xminus + xplus - 6.0 * center
        out[part, rows, :] = (-0.5 * lap + pot[0:1, :] * center).astype(out.dtype)
        return carry

    lax.fori_loop(0, parts * (orbs // step), body, 0)


def kernel(dvol, orb, pot, inter, applied, halo, panel, acc, give, take, land,
           hs, hr, ls, zs, zr, xs, xr, ds, dr, gs, gr, rs, rr):
    r, c, d = lax.axis_index("row"), lax.axis_index("col"), lax.axis_index("depth")
    parts, orbs, cells = orb.shape
    quarter = cells // 4
    half = acc.shape[2]
    peer = (r, c, 1 - d)
    zdev = [None] + [(r, flip(c, k), d) for k in (1, 2, 3)]
    xdev = [None] + [(flip(r, k), c, d) for k in (1, 2)]

    barrier = pltpu.get_barrier_semaphore()
    friends = [peer] + zdev[1:] + xdev[1:]
    for dev in friends:
        pl.semaphore_signal(barrier, inc=1, device_id=dev, device_id_type=MESH)
    pl.semaphore_wait(barrier, len(friends))

    def send(src, dst, ssem, rsem, dev):
        return pltpu.make_async_remote_copy(
            src_ref=src, dst_ref=dst, send_sem=ssem, recv_sem=rsem,
            device_id=dev, device_id_type=MESH,
        )

    def lanes(k):
        return pl.ds(pl.multiple_of(k * quarter, quarter), quarter)

    def block(j, k):
        return panel.at[j, :, pl.ds(pl.multiple_of(k * orbs, orbs), orbs), :]

    zsend = {}
    for k in (1, 3, 2):
        zsend[k] = send(orb.at[:, :, lanes(flip(c, k))], block(0, c), zs.at[k], zr.at[k], zdev[k])
        zsend[k].start()
    xsend = {}
    for j in (1, 2):
        xsend[0, j] = send(orb.at[:, :, lanes(c)], block(j, c), xs.at[0, j], xr.at[0, j], xdev[j])
        xsend[0, j].start()
    edge = send(orb, halo, hs, hr, peer)
    edge.start()
    local = pltpu.make_async_copy(orb.at[:, :, lanes(c)], block(0, c), ls)
    local.start()

    edge.wait()
    stencil(orb, halo, pot, applied)
    local.wait()

    for k in (1, 3, 2):
        zsend[k].wait_recv()
        for j in (1, 2):
            xsend[k, j] = send(block(0, flip(c, k)), block(j, flip(c, k)),
                               xs.at[k, j], xr.at[k, j], xdev[j])
            xsend[k, j].start()

    def tile(slot, jl, jr):
        for part in (0, 1):
            for mine in (0, 1):
                at = d if mine else 1 - d
                rows = pl.ds(pl.multiple_of(at * half, half), half)
                a, b = panel[jl, 0, rows, :], panel[jl, 1, rows, :]
                if part == 0:
                    s = contract(a, panel[jr, 0]) + contract(b, panel[jr, 1])
                else:
                    s = contract(a, panel[jr, 1]) - contract(b, panel[jr, 0])
                if mine:
                    acc[slot, part] = s
                else:
                    give[slot, part] = s
        cp = send(give.at[slot], take.at[slot], ds.at[slot], dr.at[slot], peer)
        cp.start()
        return cp

    def ship(t):
        to = flip(r, jnp.int32(t))
        gap = flip(c, to)
        return to, gap, send(acc.at[t], land.at[gap], gs.at[t], gr.at[gap], (r, to, d))

    def start_ship(t):
        to, gap, cp = ship(t)

        @pl.when(to != c)
        def _():
            cp.start()

    def settle(t):
        pair[t].wait_recv()
        acc[t] += take[t]

    pair = {0: tile(0, 0, 0)}
    settle(0)
    start_ship(0)
    for k in (0, 1, 3, 2):
        xsend[k, 1].wait_recv()
        xsend[k, 2].wait_recv()
    pair[4] = tile(4, 1, 2)
    pair[1] = tile(1, 0, 1)
    settle(4)
    cross = send(acc.at[4], acc.at[3], rs, rr, xdev[1])
    cross.start()
    pair[2] = tile(2, 0, 2)
    for t in (1, 2):
        settle(t)
        start_ship(t)
    cross.wait_recv()
    start_ship(3)

    total = acc[flip(r, c)]
    for k in (1, 2, 3):
        send(acc.at[0], land.at[k], gs.at[0], gr.at[k], zdev[k]).wait_recv()
        total = total + land[k]
    inter[...] = total * dvol

    for cp in [edge, cross] + list(pair.values()) + list(zsend.values()) + list(xsend.values()):
        if cp is not edge:
            cp.wait_send()
    for t in (0, 1, 2, 3):
        to, gap, cp = ship(t)

        @pl.when(to != c)
        def _():
            cp.wait_send()


def exchange(orbitals, potential):
    parts, orbs, planes, cells = orbitals.shape
    rows = orbs * lax.axis_size("col")
    half = rows // 2
    dvol = 1.0 / (planes * lax.axis_size("depth") * cells)
    vmem = pl.BlockSpec(memory_space=pltpu.VMEM)
    dma = pltpu.SemaphoreType.DMA
    inter, applied = pl.pallas_call(
        functools.partial(kernel, dvol),
        out_shape=(
            jax.ShapeDtypeStruct((2, half, rows), jnp.float32),
            jax.ShapeDtypeStruct((parts, orbs, cells), jnp.bfloat16),
        ),
        in_specs=[vmem, vmem],
        out_specs=(vmem, vmem),
        scratch_shapes=[
            pltpu.VMEM((parts, orbs, cells), jnp.bfloat16),
            pltpu.VMEM((3, parts, rows, cells // 4), jnp.bfloat16),
            pltpu.VMEM((5, 2, half, rows), jnp.float32),
            pltpu.VMEM((5, 2, half, rows), jnp.float32),
            pltpu.VMEM((5, 2, half, rows), jnp.float32),
            pltpu.VMEM((4, 2, half, rows), jnp.float32),
            dma, dma, dma, dma((4,)), dma((4,)), dma((4, 3)), dma((4, 3)),
            dma((5,)), dma((5,)), dma((4,)), dma((4,)), dma, dma,
        ],
        compiler_params=pltpu.CompilerParams(
            collective_id=0, has_side_effects=True, vmem_limit_bytes=24000000
        ),
        name="overlap",
    )(orbitals.reshape(parts, orbs, cells), potential)
    return jnp.transpose(inter, (1, 0, 2)), applied.reshape(orbitals.shape)


def solution(mesh):
    in_specs = (P(None, ("row", "col"), "depth", None), P("depth", None))
    out_specs = (P(("row", "depth"), None, "col"), P(None, ("row", "col"), "depth", None))
    sizes = tuple(mesh.shape[axis] for axis in ("row", "col", "depth"))
    body = exchange if sizes == (4, 4, 2) else shards
    return jax.shard_map(body, mesh=mesh, in_specs=in_specs, out_specs=out_specs, check_vma=False)
```

```python
import functools

import jax
import jax.numpy as jnp
from jax import lax
from jax.experimental import pallas as pl
from jax.experimental.pallas import tpu as pltpu
from jax.sharding import PartitionSpec as P

NX = 64
MESH = pl.DeviceIdType.MESH


def with_halo(block, sides, width):
    for axis, dim in sides:
        count = lax.axis_size(axis)
        forward = [(i, i + 1) for i in range(count - 1)]
        forward.append((count - 1, 0))
        backward = [(target, source) for source, target in forward]
        low = lax.ppermute(
            lax.slice_in_dim(block, block.shape[dim] - width, None, axis=dim), axis, forward
        )
        high = lax.ppermute(lax.slice_in_dim(block, 0, width, axis=dim), axis, backward)
        block = jnp.concatenate([low, block, high], axis=dim)
    return block


def apply_operator(padded, potential):
    center = padded[:, :, 1:-1].astype(jnp.float32)
    below = padded[:, :, :-2].astype(jnp.float32)
    above = padded[:, :, 2:].astype(jnp.float32)
    flat_cells = center.shape[-1]
    xpos = jnp.arange(flat_cells) % NX
    yminus = jnp.roll(center, NX, axis=3)
    yplus = jnp.roll(center, -NX, axis=3)
    xminus = jnp.where(xpos == 0, jnp.roll(center, 1 - NX, axis=3), jnp.roll(center, 1, axis=3))
    xplus = jnp.where(
        xpos == NX - 1, jnp.roll(center, NX - 1, axis=3), jnp.roll(center, -1, axis=3)
    )
    lap = below + above + yminus + yplus + xminus + xplus - 6.0 * center
    return (-0.5 * lap + potential[None, None] * center).astype(jnp.bfloat16)


def contract(left, right):
    return lax.dot_general(
        left, right, (((1,), (1,)), ((), ())), preferred_element_type=jnp.float32
    )


def shards(orbitals, potential):
    parts, orbs, planes, cells = orbitals.shape
    flat = orbitals.reshape(parts, orbs, planes * cells)
    panel = lax.all_gather(flat, "col", axis=1, tiled=True)
    other = lax.all_gather(flat, "row", axis=1, tiled=True)
    padded = with_halo(orbitals, (("depth", 2),), 1)
    applied = apply_operator(padded, potential)
    dvol = 1.0 / (planes * lax.axis_size("depth") * cells)
    tile_cols = other.shape[1]
    real_rows = panel[0]
    imag_rows = panel[1]
    sreal = contract(real_rows, other[0]) + contract(imag_rows, other[1])
    simag = contract(real_rows, other[1]) - contract(imag_rows, other[0])
    summed = lax.psum_scatter(
        dvol * jnp.concatenate([sreal, simag], axis=1), "depth", scatter_dimension=0, tiled=True
    )
    intersection = summed.reshape(summed.shape[0], 2, tile_cols)
    intersection = lax.all_to_all(intersection, "col", split_axis=2, concat_axis=2, tiled=True)
    return (intersection, applied)


def flip(a, b):
    low = lax.rem(lax.rem(a, 2) + lax.rem(b, 2), 2)
    high = lax.rem(lax.div(a, 2) + lax.div(b, 2), 2)
    return 2 * high + low


def stencil(orb, halo, pot, out):
    parts, orbs, cells = orb.shape
    step = 16
    xpos = lax.broadcasted_iota(jnp.int32, (step, cells), 1) % NX
    first, last = xpos == 0, xpos == NX - 1

    def body(i, carry):
        part = lax.div(i, orbs // step)
        rows = pl.ds(pl.multiple_of(lax.rem(i, orbs // step) * step, step), step)
        center = orb[part, rows, :].astype(jnp.float32)
        side = halo[part, rows, :].astype(jnp.float32)
        right = pltpu.roll(center, 1, 1)
        left = pltpu.roll(center, cells - 1, 1)
        yminus = pltpu.roll(center, NX, 1)
        yplus = pltpu.roll(center, cells - NX, 1)
        xminus = jnp.where(first, pltpu.roll(right, cells - NX, 1), right)
        xplus = jnp.where(last, pltpu.roll(left, NX, 1), left)
        lap = side + side + yminus + yplus + xminus + xplus - 6.0 * center
        out[part, rows, :] = (-0.5 * lap + pot[0:1, :] * center).astype(out.dtype)
        return carry

    lax.fori_loop(0, parts * (orbs // step), body, 0)


def kernel(dvol, orb_hbm, pot_hbm, inter, applied, orb, pot, halo, panel, acc, give, take,
           land, relay, ins, hs, hr, ls, zs, zr, xs, xr, ds, dr, gs, gr, qr, rs, rr):
    r, c, d = lax.axis_index("row"), lax.axis_index("col"), lax.axis_index("depth")
    parts, orbs, cells = orb.shape
    quarter = cells // 4
    half = acc.shape[2]
    load = pltpu.make_async_copy(orb_hbm, orb, ins.at[0])
    load.start()
    load_pot = pltpu.make_async_copy(pot_hbm, pot, ins.at[1])
    load_pot.start()
    peer = (r, c, 1 - d)
    zdev = [None] + [(r, flip(c, k), d) for k in (1, 2, 3)]
    xdev = [None] + [(flip(r, k), c, d) for k in (1, 2)]

    barrier = pltpu.get_barrier_semaphore()
    friends = [peer] + zdev[1:] + xdev[1:]
    for dev in friends:
        pl.semaphore_signal(barrier, inc=1, device_id=dev, device_id_type=MESH)
    load.wait()
    pl.semaphore_wait(barrier, len(friends))

    def send(src, dst, ssem, rsem, dev):
        return pltpu.make_async_remote_copy(
            src_ref=src, dst_ref=dst, send_sem=ssem, recv_sem=rsem,
            device_id=dev, device_id_type=MESH,
        )

    def lanes(k):
        return pl.ds(pl.multiple_of(k * quarter, quarter), quarter)

    def block(j, k, part):
        return panel.at[j, part, pl.ds(pl.multiple_of(k * orbs, orbs), orbs), :]

    zsend, xsend = {}, {}
    for k in (1, 3, 2):
        for p in (0, 1):
            zsend[k, p] = send(orb.at[p, :, lanes(flip(c, k))], block(0, c, p),
                               zs.at[k, p], zr.at[k, p], zdev[k])
            zsend[k, p].start()
    for p in (0, 1):
        for j in (1, 2):
            xsend[0, j, p] = send(orb.at[p, :, lanes(c)], block(j, c, p),
                                  xs.at[0, j, p], xr.at[0, j, p], xdev[j])
            xsend[0, j, p].start()
    edge = send(orb, halo, hs, hr, peer)
    edge.start()
    local = [pltpu.make_async_copy(orb.at[p, :, lanes(c)], block(0, c, p), ls.at[p])
             for p in (0, 1)]
    for cp in local:
        cp.start()

    load_pot.wait()
    edge.wait()
    stencil(orb, halo, pot, applied)
    for cp in local:
        cp.wait()

    for k in (1, 3, 2):
        for p in (0, 1):
            zsend[k, p].wait_recv()
            for j in (1, 2):
                xsend[k, j, p] = send(block(0, flip(c, k), p), block(j, flip(c, k), p),
                                      xs.at[k, j, p], xr.at[k, j, p], xdev[j])
                xsend[k, j, p].start()

    def tile(slot, jl, jr):
        a, b = panel[jl, 0], panel[jl, 1]
        for part in (0, 1):
            if part == 0:
                s = contract(a, panel[jr, 0]) + contract(b, panel[jr, 1])
            else:
                s = contract(a, panel[jr, 1]) - contract(b, panel[jr, 0])
            acc[slot, part] = jnp.where(d == 0, s[:half], s[half:])
            give[slot, part] = jnp.where(d == 0, s[half:], s[:half])
        cp = send(give.at[slot], take.at[slot], ds.at[slot], dr.at[slot], peer)
        cp.start()
        return cp

    inner = lax.rem(c + 1, 4) >= 2

    def ship(t):
        to = flip(r, jnp.int32(t))
        return to, lax.div(to, 2) != lax.div(c, 2)

    def start_ship(t):
        to, across = ship(t)

        @pl.when(jnp.logical_and(to != c, jnp.logical_not(across)))
        def _():
            send(acc.at[t], land.at[0], gs.at[t], gr.at[0], zdev[1]).start()

        @pl.when(jnp.logical_and(across, jnp.logical_not(inner)))
        def _():
            send(acc.at[t], relay.at[t], gs.at[t], qr.at[t], zdev[1]).start()

    def pass_on(t):
        to, across = ship(t)

        @pl.when(jnp.logical_and(across, inner))
        def _():
            send(acc.at[t], relay.at[t], gs.at[t], qr.at[t], zdev[1]).wait_recv()
            acc[t] += relay[t]
            send(acc.at[t], land.at[1], gs.at[t], gr.at[1], (r, to, d)).start()

    def settle(t):
        pair[t].wait_recv()
        acc[t] += take[t]

    pair = {0: tile(0, 0, 0)}
    settle(0)
    start_ship(0)
    for k in (0, 1, 3, 2):
        for j in (1, 2):
            for p in (0, 1):
                xsend[k, j, p].wait_recv()
    pair[4] = tile(4, 1, 2)
    pair[1] = tile(1, 0, 1)
    settle(4)
    cross = send(acc.at[4], acc.at[3], rs, rr, xdev[1])
    cross.start()
    settle(1)
    start_ship(1)
    pair[2] = tile(2, 0, 2)
    pass_on(0)
    settle(2)
    start_ship(2)
    pass_on(1)
    cross.wait_recv()
    start_ship(3)
    pass_on(2)
    pass_on(3)

    total = acc[flip(r, c)]
    for k in (0, 1):
        send(acc.at[0], land.at[k], gs.at[0], gr.at[k], zdev[1]).wait_recv()
        total = total + land[k]
    inter[...] = total * dvol

    for cp in [edge, cross] + list(pair.values()) + list(zsend.values()) + list(xsend.values()):
        if cp is not edge:
            cp.wait_send()
    for t in (0, 1, 2, 3):
        to, across = ship(t)

        @pl.when(to != c)
        def _():
            send(acc.at[t], land.at[0], gs.at[t], gr.at[0], zdev[1]).wait_send()


def exchange(orbitals, potential):
    parts, orbs, planes, cells = orbitals.shape
    rows = orbs * lax.axis_size("col")
    half = rows // 2
    dvol = 1.0 / (planes * lax.axis_size("depth") * cells)
    vmem = pl.BlockSpec(memory_space=pltpu.VMEM)
    dma = pltpu.SemaphoreType.DMA
    inter, applied = pl.pallas_call(
        functools.partial(kernel, dvol),
        out_shape=(
            jax.ShapeDtypeStruct((2, half, rows), jnp.float32),
            jax.ShapeDtypeStruct((parts, orbs, cells), jnp.bfloat16),
        ),
        in_specs=[pl.BlockSpec(memory_space=pltpu.HBM)] * 2,
        out_specs=(vmem, vmem),
        scratch_shapes=[
            pltpu.VMEM((parts, orbs, cells), jnp.bfloat16),
            pltpu.VMEM(potential.shape, jnp.float32),
            pltpu.VMEM((parts, orbs, cells), jnp.bfloat16),
            pltpu.VMEM((3, parts, rows, cells // 4), jnp.bfloat16),
            pltpu.VMEM((5, 2, half, rows), jnp.float32),
            pltpu.VMEM((5, 2, half, rows), jnp.float32),
            pltpu.VMEM((5, 2, half, rows), jnp.float32),
            pltpu.VMEM((2, 2, half, rows), jnp.float32),
            pltpu.VMEM((4, 2, half, rows), jnp.float32),
            dma((2,)), dma, dma, dma((2,)), dma((4, 2)), dma((4, 2)), dma((4, 3, 2)),
            dma((4, 3, 2)), dma((5,)), dma((5,)), dma((4,)), dma((2,)), dma((4,)), dma, dma,
        ],
        compiler_params=pltpu.CompilerParams(
            collective_id=0, has_side_effects=True, vmem_limit_bytes=24000000
        ),
        name="overlap",
    )(orbitals.reshape(parts, orbs, cells), potential)
    return jnp.transpose(inter, (1, 0, 2)), applied.reshape(orbitals.shape)


def solution(mesh):
    in_specs = (P(None, ("row", "col"), "depth", None), P("depth", None))
    out_specs = (P(("row", "depth"), None, "col"), P(None, ("row", "col"), "depth", None))
    sizes = tuple(mesh.shape[axis] for axis in ("row", "col", "depth"))
    body = exchange if sizes == (4, 4, 2) else shards
    return jax.shard_map(body, mesh=mesh, in_specs=in_specs, out_specs=out_specs, check_vma=False)
```

```python
import functools

import jax
import jax.numpy as jnp
from jax import lax
from jax.experimental import pallas as pl
from jax.experimental.pallas import tpu as pltpu
from jax.sharding import PartitionSpec as P

NX = 64
MESH = pl.DeviceIdType.MESH


def with_halo(block, sides, width):
    for axis, dim in sides:
        count = lax.axis_size(axis)
        forward = [(i, i + 1) for i in range(count - 1)]
        forward.append((count - 1, 0))
        backward = [(target, source) for source, target in forward]
        low = lax.ppermute(
            lax.slice_in_dim(block, block.shape[dim] - width, None, axis=dim), axis, forward
        )
        high = lax.ppermute(lax.slice_in_dim(block, 0, width, axis=dim), axis, backward)
        block = jnp.concatenate([low, block, high], axis=dim)
    return block


def apply_operator(padded, potential):
    center = padded[:, :, 1:-1].astype(jnp.float32)
    below = padded[:, :, :-2].astype(jnp.float32)
    above = padded[:, :, 2:].astype(jnp.float32)
    flat_cells = center.shape[-1]
    xpos = jnp.arange(flat_cells) % NX
    yminus = jnp.roll(center, NX, axis=3)
    yplus = jnp.roll(center, -NX, axis=3)
    xminus = jnp.where(xpos == 0, jnp.roll(center, 1 - NX, axis=3), jnp.roll(center, 1, axis=3))
    xplus = jnp.where(
        xpos == NX - 1, jnp.roll(center, NX - 1, axis=3), jnp.roll(center, -1, axis=3)
    )
    lap = below + above + yminus + yplus + xminus + xplus - 6.0 * center
    return (-0.5 * lap + potential[None, None] * center).astype(jnp.bfloat16)


def contract(left, right):
    return lax.dot_general(
        left, right, (((1,), (1,)), ((), ())), preferred_element_type=jnp.float32
    )


def shards(orbitals, potential):
    parts, orbs, planes, cells = orbitals.shape
    flat = orbitals.reshape(parts, orbs, planes * cells)
    panel = lax.all_gather(flat, "col", axis=1, tiled=True)
    other = lax.all_gather(flat, "row", axis=1, tiled=True)
    padded = with_halo(orbitals, (("depth", 2),), 1)
    applied = apply_operator(padded, potential)
    dvol = 1.0 / (planes * lax.axis_size("depth") * cells)
    tile_cols = other.shape[1]
    real_rows = panel[0]
    imag_rows = panel[1]
    sreal = contract(real_rows, other[0]) + contract(imag_rows, other[1])
    simag = contract(real_rows, other[1]) - contract(imag_rows, other[0])
    summed = lax.psum_scatter(
        dvol * jnp.concatenate([sreal, simag], axis=1), "depth", scatter_dimension=0, tiled=True
    )
    intersection = summed.reshape(summed.shape[0], 2, tile_cols)
    intersection = lax.all_to_all(intersection, "col", split_axis=2, concat_axis=2, tiled=True)
    return (intersection, applied)


def flip(a, b):
    low = lax.rem(lax.rem(a, 2) + lax.rem(b, 2), 2)
    high = lax.rem(lax.div(a, 2) + lax.div(b, 2), 2)
    return 2 * high + low


def stencil(orb, halo, pot, out):
    parts, orbs, cells = orb.shape
    step = 16
    xpos = lax.broadcasted_iota(jnp.int32, (step, cells), 1) % NX
    first, last = xpos == 0, xpos == NX - 1

    def body(i, carry):
        part = lax.div(i, orbs // step)
        rows = pl.ds(pl.multiple_of(lax.rem(i, orbs // step) * step, step), step)
        center = orb[part, rows, :].astype(jnp.float32)
        side = halo[part, rows, :].astype(jnp.float32)
        right = pltpu.roll(center, 1, 1)
        left = pltpu.roll(center, cells - 1, 1)
        yminus = pltpu.roll(center, NX, 1)
        yplus = pltpu.roll(center, cells - NX, 1)
        xminus = jnp.where(first, pltpu.roll(right, cells - NX, 1), right)
        xplus = jnp.where(last, pltpu.roll(left, NX, 1), left)
        lap = side + side + yminus + yplus + xminus + xplus - 6.0 * center
        out[part, rows, :] = (-0.5 * lap + pot[0:1, :] * center).astype(out.dtype)
        return carry

    lax.fori_loop(0, parts * (orbs // step), body, 0)


def kernel(dvol, orb_hbm, pot_hbm, inter, applied, orb, pot, halo, panel, acc, give, take,
           land, relay, ins, hs, hr, ls, zs, zr, xs, xr, ds, dr, gs, gr, qr, rs, rr):
    r, c, d = lax.axis_index("row"), lax.axis_index("col"), lax.axis_index("depth")
    parts, orbs, cells = orb.shape
    quarter = cells // 4
    half = acc.shape[2]
    load = pltpu.make_async_copy(orb_hbm, orb, ins.at[0])
    load.start()
    load_pot = pltpu.make_async_copy(pot_hbm, pot, ins.at[1])
    load_pot.start()
    peer = (r, c, 1 - d)
    zdev = [None] + [(r, flip(c, k), d) for k in (1, 2, 3)]
    xdev = [None] + [(flip(r, k), c, d) for k in (1, 2)]

    barrier = pltpu.get_barrier_semaphore()
    friends = [peer] + zdev[1:] + xdev[1:]
    for dev in friends:
        pl.semaphore_signal(barrier, inc=1, device_id=dev, device_id_type=MESH)
    load.wait()
    pl.semaphore_wait(barrier, len(friends))

    def send(src, dst, ssem, rsem, dev):
        return pltpu.make_async_remote_copy(
            src_ref=src, dst_ref=dst, send_sem=ssem, recv_sem=rsem,
            device_id=dev, device_id_type=MESH,
        )

    def lanes(k):
        return pl.ds(pl.multiple_of(k * quarter, quarter), quarter)

    def block(j, k, part):
        return panel.at[j, part, pl.ds(pl.multiple_of(k * orbs, orbs), orbs), :]

    zsend, xsend = {}, {}
    for k in (1, 3, 2):
        for p in (0, 1):
            zsend[k, p] = send(orb.at[p, :, lanes(flip(c, k))], block(0, c, p),
                               zs.at[k, p], zr.at[k, p], zdev[k])
            zsend[k, p].start()
    for p in (0, 1):
        for j in (1, 2):
            xsend[0, j, p] = send(orb.at[p, :, lanes(c)], block(j, c, p),
                                  xs.at[0, j, p], xr.at[0, j, p], xdev[j])
            xsend[0, j, p].start()
    edge = send(orb, halo, hs, hr, peer)
    edge.start()
    local = [pltpu.make_async_copy(orb.at[p, :, lanes(c)], block(0, c, p), ls.at[p])
             for p in (0, 1)]
    for cp in local:
        cp.start()

    load_pot.wait()
    edge.wait()
    stencil(orb, halo, pot, applied)
    for cp in local:
        cp.wait()

    for k in (1, 3, 2):
        for p in (0, 1):
            zsend[k, p].wait_recv()
            for j in (1, 2):
                xsend[k, j, p] = send(block(0, flip(c, k), p), block(j, flip(c, k), p),
                                      xs.at[k, j, p], xr.at[k, j, p], xdev[j])
                xsend[k, j, p].start()

    def tile(slot, jl, jr):
        for part in (0, 1):
            if slot == 4 and part == 1:
                jl, jr = jr, jl
            a, b = panel[jl, 0], panel[jl, 1]
            if part == 0:
                s = contract(a, panel[jr, 0]) + contract(b, panel[jr, 1])
            else:
                s = contract(a, panel[jr, 1]) - contract(b, panel[jr, 0])
            acc[slot, part] = jnp.where(d == 0, s[:half], s[half:])
            give[slot, part] = jnp.where(d == 0, s[half:], s[:half])
        cp = send(give.at[slot], take.at[slot], ds.at[slot], dr.at[slot], peer)
        cp.start()
        return cp

    inner = lax.rem(c + 1, 4) >= 2

    def ship(t):
        to = flip(r, jnp.int32(t))
        return to, lax.div(to, 2) != lax.div(c, 2)

    def start_ship(t):
        to, across = ship(t)

        @pl.when(jnp.logical_and(to != c, jnp.logical_not(across)))
        def _():
            send(acc.at[t], land.at[0], gs.at[t], gr.at[0], zdev[1]).start()

        @pl.when(jnp.logical_and(across, jnp.logical_not(inner)))
        def _():
            send(acc.at[t], relay.at[t], gs.at[t], qr.at[t], zdev[1]).start()

    def pass_on(t):
        to, across = ship(t)

        @pl.when(jnp.logical_and(across, inner))
        def _():
            send(acc.at[t], relay.at[t], gs.at[t], qr.at[t], zdev[1]).wait_recv()
            acc[t] += relay[t]
            send(acc.at[t], land.at[1], gs.at[t], gr.at[1], (r, to, d)).start()

    def settle(t):
        pair[t].wait_recv()
        acc[t] += take[t]

    pair = {0: tile(0, 0, 0)}
    settle(0)
    start_ship(0)
    for k in (0, 1, 3, 2):
        for j in (1, 2):
            for p in (0, 1):
                xsend[k, j, p].wait_recv()
    pair[4] = tile(4, 1, 2)
    pair[2] = tile(2, 0, 2)
    settle(4)
    cross = [send(acc.at[4, p], acc.at[3, p], rs.at[p], rr.at[p], xdev[1 + p]) for p in (0, 1)]
    for cp in cross:
        cp.start()
    settle(2)
    start_ship(2)
    pair[1] = tile(1, 0, 1)
    pass_on(0)
    settle(1)
    for cp in cross:
        cp.wait_recv()
    start_ship(3)
    start_ship(1)
    pass_on(2)
    pass_on(3)
    pass_on(1)

    total = acc[flip(r, c)]
    for k in (0, 1):
        send(acc.at[0], land.at[k], gs.at[0], gr.at[k], zdev[1]).wait_recv()
        total = total + land[k]
    inter[...] = total * dvol

    for cp in [edge] + cross + list(pair.values()) + list(zsend.values()) + list(xsend.values()):
        if cp is not edge:
            cp.wait_send()
    for t in (0, 1, 2, 3):
        to, across = ship(t)

        @pl.when(to != c)
        def _():
            send(acc.at[t], land.at[0], gs.at[t], gr.at[0], zdev[1]).wait_send()


def exchange(orbitals, potential):
    parts, orbs, planes, cells = orbitals.shape
    rows = orbs * lax.axis_size("col")
    half = rows // 2
    dvol = 1.0 / (planes * lax.axis_size("depth") * cells)
    vmem = pl.BlockSpec(memory_space=pltpu.VMEM)
    dma = pltpu.SemaphoreType.DMA
    inter, applied = pl.pallas_call(
        functools.partial(kernel, dvol),
        out_shape=(
            jax.ShapeDtypeStruct((2, half, rows), jnp.float32),
            jax.ShapeDtypeStruct((parts, orbs, cells), jnp.bfloat16),
        ),
        in_specs=[pl.BlockSpec(memory_space=pltpu.HBM)] * 2,
        out_specs=(vmem, vmem),
        scratch_shapes=[
            pltpu.VMEM((parts, orbs, cells), jnp.bfloat16),
            pltpu.VMEM(potential.shape, jnp.float32),
            pltpu.VMEM((parts, orbs, cells), jnp.bfloat16),
            pltpu.VMEM((3, parts, rows, cells // 4), jnp.bfloat16),
            pltpu.VMEM((5, 2, half, rows), jnp.float32),
            pltpu.VMEM((5, 2, half, rows), jnp.float32),
            pltpu.VMEM((5, 2, half, rows), jnp.float32),
            pltpu.VMEM((2, 2, half, rows), jnp.float32),
            pltpu.VMEM((4, 2, half, rows), jnp.float32),
            dma((2,)), dma, dma, dma((2,)), dma((4, 2)), dma((4, 2)), dma((4, 3, 2)),
            dma((4, 3, 2)), dma((5,)), dma((5,)), dma((4,)), dma((2,)), dma((4,)), dma((2,)), dma((2,)),
        ],
        compiler_params=pltpu.CompilerParams(
            collective_id=0, has_side_effects=True, vmem_limit_bytes=24000000
        ),
        name="overlap",
    )(orbitals.reshape(parts, orbs, cells), potential)
    return jnp.transpose(inter, (1, 0, 2)), applied.reshape(orbitals.shape)


def solution(mesh):
    in_specs = (P(None, ("row", "col"), "depth", None), P("depth", None))
    out_specs = (P(("row", "depth"), None, "col"), P(None, ("row", "col"), "depth", None))
    sizes = tuple(mesh.shape[axis] for axis in ("row", "col", "depth"))
    body = exchange if sizes == (4, 4, 2) else shards
    return jax.shard_map(body, mesh=mesh, in_specs=in_specs, out_specs=out_specs, check_vma=False)
```
